8 devices in a mesh: dp: 2 (over z, y), pp: 4 (over x, core).
Axes of the slice: x: 2, y: 2, z: 1, core: 2. Of those that a mesh axis runs over, the one named last changes fastest.
Arguments:
- tok_ids: int32 [2, 2, 130], P(None, 'dp')
- emb_s: bfloat16 [4, 50304, 2048], P('pp', 'dp')
- w_one: bfloat16 [4, 1, 2048, 8192], P('pp')
- w_two: bfloat16 [4, 1, 8192, 2048], P('pp')
- gain_f: bfloat16 [2048], replicated
- gain_h: bfloat16 [2048], replicated
- gain_e: bfloat16 [2048], replicated
- gain_m: bfloat16 [2048], replicated
- w_proj: bfloat16 [4096, 2048], replicated
- u_one: bfloat16 [2048, 8192], replicated
- u_two: bfloat16 [8192, 2048], replicated
- w_out: bfloat16 [2048, 50304], replicated
Outputs:
- output 1: float32 [], replicated
- output 2: float32 [2, 2, 128], P(None, 'dp')
- output 3: float32 [2, 2, 128], P(None, 'dp')
All inputs are finite; a program needn't handle non-finite values.
Results may differ from the reference program's by a relative error of at most 0.00315102.
Values are sent between devices in bfloat16 or wider.
A program may use at most 1.75 GiB of HBM per device.

```python
import jax
import jax.numpy as jnp
from jax import lax

STAGES = 4
LAYERS = 1
MICRO_BATCHES = 2
GLOBAL_BATCH = 2
SEQ_LEN = 128
HIDDEN = 2048
FFN_HIDDEN = 8192
VOCAB_SIZE = 50304
HEAD_ROWS = 128
NORM_EPS = 1e-6
MTP_WEIGHT = 0.3


def setup_inputs(seed: int = 0) -> dict:
    key_list = jax.random.split(jax.random.key(seed), 12)
    tok_ids = jax.random.randint(key_list[0], (MICRO_BATCHES, GLOBAL_BATCH, SEQ_LEN + 2), 0, VOCAB_SIZE, dtype=jnp.int32)
    tok_ids = tok_ids.at[0, 0, 0].set(0).at[0, 0, 1].set(VOCAB_SIZE - 1)
    table = jax.random.normal(key_list[1], (VOCAB_SIZE, HIDDEN), jnp.float32).astype(jnp.bfloat16)
    emb_s = jnp.concatenate([table[None], jnp.zeros((STAGES - 1, VOCAB_SIZE, HIDDEN), jnp.bfloat16)], axis=0)
    w_one = (jax.random.normal(key_list[2], (STAGES, LAYERS, HIDDEN, FFN_HIDDEN), jnp.float32) * HIDDEN ** -0.5).astype(jnp.bfloat16)
    w_two = (jax.random.normal(key_list[3], (STAGES, LAYERS, FFN_HIDDEN, HIDDEN), jnp.float32) * FFN_HIDDEN ** -0.5).astype(jnp.bfloat16)
    gain_f = jax.random.uniform(key_list[4], (HIDDEN,), jnp.float32, 0.25, 1.75).astype(jnp.bfloat16)
    gain_h = jax.random.uniform(key_list[5], (HIDDEN,), jnp.float32, 0.25, 1.75).astype(jnp.bfloat16)
    gain_e = jax.random.uniform(key_list[6], (HIDDEN,), jnp.float32, 0.25, 1.75).astype(jnp.bfloat16)
    gain_m = jax.random.uniform(key_list[7], (HIDDEN,), jnp.float32, 0.25, 1.75).astype(jnp.bfloat16)
    w_proj = (jax.random.normal(key_list[8], (2 * HIDDEN, HIDDEN), jnp.float32) * (2 * HIDDEN) ** -0.5).astype(jnp.bfloat16)
    u_one = (jax.random.normal(key_list[9], (HIDDEN, FFN_HIDDEN), jnp.float32) * HIDDEN ** -0.5).astype(jnp.bfloat16)
    u_two = (jax.random.normal(key_list[10], (FFN_HIDDEN, HIDDEN), jnp.float32) * FFN_HIDDEN ** -0.5).astype(jnp.bfloat16)
    w_out = (jax.random.normal(key_list[11], (HIDDEN, VOCAB_SIZE), jnp.float32) * 3.0 * HIDDEN ** -0.5).astype(jnp.bfloat16)
    return {'tok_ids': tok_ids, 'emb_s': emb_s, 'w_one': w_one, 'w_two': w_two, 'gain_f': gain_f, 'gain_h': gain_h, 'gain_e': gain_e, 'gain_m': gain_m, 'w_proj': w_proj, 'u_one': u_one, 'u_two': u_two, 'w_out': w_out}


def norm_plain(x_val):
    x_f = x_val.astype(jnp.float32)
    return (x_f * lax.rsqrt(jnp.mean(x_f * x_f, axis=-1, keepdims=True) + NORM_EPS)).astype(jnp.bfloat16)


def norm_gain(x_val, gain_vec):
    x_f = x_val.astype(jnp.float32)
    scaled = x_f * lax.rsqrt(jnp.mean(x_f * x_f, axis=-1, keepdims=True) + NORM_EPS)
    return (scaled * gain_vec.astype(jnp.float32)).astype(jnp.bfloat16)


def mlp_add(x_val, normed, w_up, w_down):
    hidden = jax.nn.gelu(jnp.dot(normed, w_up, preferred_element_type=jnp.float32)).astype(jnp.bfloat16)
    return (x_val.astype(jnp.float32) + jnp.dot(hidden, w_down, preferred_element_type=jnp.float32)).astype(jnp.bfloat16)


def row_nll(normed, targets, w_out):
    n_blocks = normed.shape[0] // HEAD_ROWS

    def one_block(pair):
        block_rows, block_tgt = pair
        logits = jnp.dot(block_rows, w_out, preferred_element_type=jnp.float32)
        picked = jnp.take_along_axis(logits, block_tgt[:, None], axis=1)[:, 0]
        return jax.nn.logsumexp(logits, axis=1) - picked

    per_block = lax.map(one_block, (normed.reshape(n_blocks, HEAD_ROWS, HIDDEN), targets.reshape(n_blocks, HEAD_ROWS)))
    return per_block.reshape(n_blocks * HEAD_ROWS)


def reference(tok_ids, emb_s, w_one, w_two, gain_f, gain_h, gain_e, gain_m, w_proj, u_one, u_two, w_out):
    table = emb_s[0]
    w_up = w_one.reshape(STAGES * LAYERS, HIDDEN, FFN_HIDDEN)
    w_down = w_two.reshape(STAGES * LAYERS, FFN_HIDDEN, HIDDEN)
    seqs = tok_ids.reshape(MICRO_BATCHES * GLOBAL_BATCH, SEQ_LEN + 2)

    def layer_step(x_val, weights):
        w_a, w_b = weights
        return mlp_add(x_val, norm_plain(x_val), w_a, w_b), None

    def per_sequence(ids):
        x_val = table[ids[:SEQ_LEN]]
        h_last, _ = lax.scan(layer_step, x_val, (w_up, w_down))
        main_nll = row_nll(norm_gain(h_last, gain_f), ids[1:SEQ_LEN + 1], w_out)
        e_rows = table[ids[1:SEQ_LEN + 1]]
        joined = jnp.concatenate([norm_gain(h_last, gain_h), norm_gain(e_rows, gain_e)], axis=1)
        z_val = jnp.dot(joined, w_proj, preferred_element_type=jnp.float32).astype(jnp.bfloat16)
        z_val = mlp_add(z_val, norm_gain(z_val, gain_m), u_one, u_two)
        mtp_nll = row_nll(norm_gain(z_val, gain_f), ids[2:], w_out)
        return main_nll, mtp_nll

    main_nll, mtp_nll = lax.map(per_sequence, seqs)
    main_nll = main_nll.reshape(MICRO_BATCHES, GLOBAL_BATCH, SEQ_LEN)
    mtp_nll = mtp_nll.reshape(MICRO_BATCHES, GLOBAL_BATCH, SEQ_LEN)
    total_loss = jnp.mean(main_nll) + MTP_WEIGHT * jnp.mean(mtp_nll)
    return (total_loss, main_nll, mtp_nll)
```

```python
import functools

import jax
import jax.numpy as jnp
from jax import lax
from jax.experimental import pallas as pl
from jax.experimental.pallas import tpu as pltpu
from jax.sharding import PartitionSpec as P

NORM_EPS = 1e-6
MTP_WEIGHT = 0.3
LANES = 128
NEG = -3.0e38
CHUNK = 1024
HALF = 512
N_SLOTS = 12
MESH = pl.DeviceIdType.MESH
GROUP = 8


def gather_kernel(n_ids, flag_ref, grp_ref, sel_ref, table_ref, out_ref, buf, sems):
    n_batches = buf.shape[0]

    def start(batch):
        def one(j, carry):
            first = pl.multiple_of(grp_ref[batch * n_ids + j] * GROUP, GROUP)
            pltpu.make_async_copy(
                table_ref.at[pl.ds(first, GROUP), :], buf.at[batch, j], sems.at[batch]
            ).start()
            return carry

        lax.fori_loop(0, n_ids, one, 0, unroll=43)

    @pl.when(flag_ref[0] == 0)
    def _():
        for batch in range(n_batches):
            start(batch)
        col = lax.broadcasted_iota(jnp.int32, (out_ref.shape[1], n_ids * GROUP), 1)
        for batch in range(n_batches):
            pltpu.make_async_copy(buf.at[batch], buf.at[batch], sems.at[batch]).wait()
            hot = jnp.where(col == sel_ref[batch], 1.0, 0.0).astype(jnp.bfloat16)
            rows = buf[batch].reshape(n_ids * GROUP, -1)
            out_ref[batch] = jnp.dot(hot, rows, preferred_element_type=jnp.float32).astype(jnp.bfloat16)


def gather_rows(flag, local, owned, table):
    n_batches, n_ids = local.shape
    n_out = pl.cdiv(n_ids, GROUP) * GROUP
    width = table.shape[1]
    grp = local // GROUP
    sub = local - grp * GROUP
    sel = jnp.where(owned, jnp.arange(n_ids, dtype=jnp.int32) * GROUP + sub, -1)
    sel = jnp.pad(sel, ((0, 0), (0, n_out - n_ids)), constant_values=-1)
    return pl.pallas_call(
        functools.partial(gather_kernel, n_ids),
        grid_spec=pltpu.PrefetchScalarGridSpec(
            num_scalar_prefetch=2,
            grid=(),
            in_specs=[pl.BlockSpec(memory_space=pltpu.VMEM), pl.BlockSpec(memory_space=pl.ANY)],
            out_specs=pl.BlockSpec(memory_space=pltpu.VMEM),
            scratch_shapes=[
                pltpu.VMEM((n_batches, n_ids, GROUP, width), table.dtype),
                pltpu.SemaphoreType.DMA((n_batches,)),
            ],
        ),
        out_shape=jax.ShapeDtypeStruct((n_batches, n_out, width), table.dtype),
        compiler_params=pltpu.CompilerParams(vmem_limit_bytes=40 << 20),
        name="gather_rows",
    )(flag.reshape(1), grp.reshape(-1), sel[..., None], table)


def scaled_rows(rows, gain):
    x_f = rows.astype(jnp.float32)
    y = x_f * lax.rsqrt(jnp.mean(x_f * x_f, axis=-1, keepdims=True) + NORM_EPS)
    if gain is not None:
        y = y * gain
    return y.astype(jnp.bfloat16)


def norm_into(dst, src, gain_ref=None):
    gain = None if gain_ref is None else gain_ref[...].astype(jnp.float32).reshape(1, -1)
    for r in range(0, src.shape[0], 16):
        dst[pl.ds(r, 16), :] = scaled_rows(src[pl.ds(r, 16), :], gain)


def gelu(y):
    inner = y * (0.7978845608028654 + (0.7978845608028654 * 0.044715) * (y * y))
    return (y * (0.5 + 0.5 * jnp.tanh(inner))).astype(jnp.bfloat16)


def dot(a, b):
    return jnp.dot(a, b, preferred_element_type=jnp.float32)


def mega_kernel(
    rows, tgt, gain_f, gain_h, gain_e, gain_m, w_one, w_two, w_proj, u_one, u_two, w_out,
    out, wbuf, x_in, hid, x_out, h_buf, e_buf, n_buf, top, total, pick, stat,
    wsem, loc_sem, xs_sem, xr_sem, ex_s, ex_r, es_sem, er_sem, hs_sem, hs2_sem, hr_sem, rl_sem, zs_sem, zs2_sem, zr_sem, zl_sem, ss_sem, sr_sem,
):
    role = lax.axis_index('pp')
    dp = lax.axis_index('dp')
    n_roles, n_data = 4, 2
    n_dev = n_roles * n_data
    me = dp * n_roles + role
    n_vocab = w_out.shape[1]
    width = x_in.shape[2]
    n_half = n_buf.shape[1] // 2
    n_rows = n_buf.shape[1]
    n_cols = pl.cdiv(n_vocab, CHUNK)
    xn = n_buf.at[0, pl.ds(0, n_half)]
    body_rows = pl.ds(0, n_half)
    z_buf = x_in
    last_role = n_roles - 1
    last = role == last_role
    lane_main = jnp.where(role == 0, 0, jnp.where(role == 2, 1, 2))
    n_main = jnp.where(last, 0, (n_cols - lane_main + 2) // 3)
    n_mtp = (n_cols - role + 3) // 4
    q_mtp = jnp.where(last, 20, n_main)
    q_end = q_mtp + n_mtp

    def load(src, slot):
        pltpu.make_async_copy(src, wbuf.at[slot], wsem.at[slot]).start()

    def wait_slot(slot):
        pltpu.make_async_copy(w_proj.at[pl.ds(0, width), pl.ds(0, CHUNK)], wbuf.at[slot], wsem.at[slot]).wait()

    def cols(c):
        return pl.ds(pl.multiple_of(c * CHUNK, CHUNK), CHUNK)

    def rows_at(k):
        return pl.ds(pl.multiple_of(k * width, width), width)

    def up_chunk(c):
        return w_one.at[0, 0, :, cols(c)]

    def down_chunk(g, k):
        return w_two.at[0, 0, rows_at(k), cols(g)]

    def head_col(q):
        return jnp.where(q < n_main, lane_main + 3 * q, role + 4 * (q - q_mtp))

    def head_start(col):
        return pl.multiple_of(jnp.minimum(col * CHUNK, n_vocab - CHUNK), LANES)

    def issue_post(q):
        slot = lax.rem(q, N_SLOTS)

        @pl.when(((q < n_main) | (q >= q_mtp)) & (q < q_end))
        def _():
            load(w_out.at[:, pl.ds(head_start(head_col(q)), CHUNK)], slot)

        @pl.when(last & (q < 4))
        def _():
            load(w_proj.at[rows_at(lax.rem(q, 2)), cols(q // 2)], slot)

        @pl.when(last & (q >= 4) & (q < 12))
        def _():
            load(u_one.at[:, cols(q - 4)], slot)

        @pl.when(last & (q >= 12) & (q < 20))
        def _():
            load(u_two.at[rows_at(lax.rem(q - 12, 4)), cols((q - 12) // 4)], slot)

    def remote(src, dst, send, recv, to_dp, to_pp):
        return pltpu.make_async_remote_copy(
            src_ref=src, dst_ref=dst, send_sem=send, recv_sem=recv, device_id=(to_dp, to_pp), device_id_type=MESH
        )

    for c in range(8):
        load(up_chunk(c), c // 2 if c % 2 == 0 else 8 + (c // 2))
    for c in range(4):
        load(down_chunk(c // 2, 2 * (c % 2)), 4 + c)

    barrier = pltpu.get_barrier_semaphore()
    for o in range(1, n_dev):
        peer = lax.rem(me + o, n_dev)
        pl.semaphore_signal(barrier, inc=1, device_id=(peer // n_roles, lax.rem(peer, n_roles)), device_id_type=MESH)
    pl.semaphore_wait(barrier, n_dev - 1)

    def exchange(mb):
        return remote(rows.at[2 + mb], x_in.at[mb], ex_s.at[mb], ex_r.at[mb], 1 - dp, 0)

    def local_rows(mb):
        return pltpu.make_async_copy(rows.at[mb], x_out.at[mb], loc_sem.at[mb])

    @pl.when(role == 0)
    def _():
        for mb in range(2):
            exchange(mb).start()
        for mb in range(2):
            local_rows(mb).start()

    def piece(ref, mb, g):
        return ref.at[mb, body_rows, cols(g)]

    def hand_on(mb, g):
        i = 2 * mb + g
        return remote(piece(x_out, mb, g), piece(x_in, mb, g), xs_sem.at[i], xr_sem.at[i], dp, jnp.minimum(role + 1, last_role))

    def h_to_one(mb, g):
        i = 2 * mb + g
        return remote(piece(x_out, mb, g), piece(h_buf, mb, g), hs_sem.at[i], hr_sem.at[i], dp, 1)

    def h_to_two(mb, g):
        i = 2 * mb + g
        return remote(piece(x_out, mb, g), piece(h_buf, mb, g), hs2_sem.at[i], hr_sem.at[i], dp, 2)

    def h_relay(mb, g):
        i = 2 * mb + g
        return remote(piece(h_buf, mb, g), piece(h_buf, mb, g), rl_sem.at[i], hr_sem.at[i], dp, 0)

    def e_on(mb):
        return remote(x_in.at[mb], e_buf.at[mb], es_sem.at[mb], er_sem.at[mb], dp, last_role)

    def stage_pass(mb, carry):
        @pl.when(role == 0)
        def _():
            local_rows(mb).wait()
            exchange(mb).wait_recv()
            for r in range(0, x_in.shape[1], 8):
                at = pl.ds(r, 8)
                x_in[mb, at, :] = x_in[mb, at, :] + x_out[mb, at, :]

        @pl.when(role > 0)
        def _():
            for g in range(2):
                hand_on(mb, g).wait_recv()

        norm_into(xn, x_in.at[mb, body_rows])

        @pl.when(role == 0)
        def _():
            e_on(mb).start()

        def up(i, c2):
            @pl.when(mb == 0)
            def _():
                wait_slot(i)

            wait_slot(8 + i)
            for e, slot in ((0, i), (1, 8 + i)):
                for n in range(0, CHUNK, HALF):
                    y = dot(xn[...], wbuf[slot, :, pl.ds(n, HALF)])
                    at = pl.multiple_of((2 * i + e) * CHUNK + n, HALF)
                    hid[pl.ds(0, n_half), pl.ds(at, HALF)] = gelu(y)
            g2 = i // 2
            load(down_chunk(g2, 2 * lax.rem(i, 2) + 1), 8 + i)

            @pl.when(mb == 1)
            def _():
                issue_post(i)

            return c2

        lax.fori_loop(0, 4, up, 0)

        def down(g, c2):
            @pl.when(mb == 0)
            def _():
                wait_slot(4 + 2 * g)
                wait_slot(5 + 2 * g)

            wait_slot(8 + 2 * g)
            wait_slot(9 + 2 * g)
            slots = (4 + 2 * g, 8 + 2 * g, 5 + 2 * g, 9 + 2 * g)
            for n in range(0, CHUNK, HALF):
                y = None
                for k in range(4):
                    part = dot(hid[pl.ds(0, n_half), pl.ds(k * width, width)], wbuf[slots[k], :, pl.ds(n, HALF)])
                    y = part if y is None else y + part
                at = pl.ds(pl.multiple_of(g * CHUNK + n, HALF), HALF)
                x_out[mb, body_rows, at] = (x_in[mb, body_rows, at].astype(jnp.float32) + y).astype(jnp.bfloat16)

            @pl.when(mb == 0)
            def _():
                load(up_chunk(4 * g + 1), 8 + 2 * g)
                load(up_chunk(4 * g + 3), 9 + 2 * g)

            @pl.when(mb == 1)
            def _():
                issue_post(4 + 2 * g)
                issue_post(5 + 2 * g)
                issue_post(8 + 2 * g)
                issue_post(9 + 2 * g)

            @pl.when((role == 0) & (g == 1))
            def _():
                e_on(mb).wait_send()

            @pl.when(role < last_role)
            def _():
                hand_on(mb, g).start()

            @pl.when(last)
            def _():
                h_to_one(mb, g).start()
                h_to_two(mb, g).start()

            return c2

        lax.fori_loop(0, 2, down, 0)
        return carry

    lax.fori_loop(0, 2, stage_pass, 0)

    def z_piece(g):
        return z_buf.at[:, body_rows, cols(g)]

    def z_to_one(g):
        return remote(z_piece(g), z_piece(g), zs_sem.at[g], zr_sem.at[g], dp, 1)

    def z_to_two(g):
        return remote(z_piece(g), z_piece(g), zs2_sem.at[g], zr_sem.at[g], dp, 2)

    def z_relay(g):
        return remote(z_piece(g), z_piece(g), zl_sem.at[g], zr_sem.at[g], dp, 0)

    @pl.when(role < last_role)
    def _():
        for mb in range(2):
            for g in range(2):
                h_to_one(mb, g).wait_recv()

                @pl.when(role == 1)
                def _():
                    h_relay(mb, g).start()

        for mb in range(2):
            norm_into(n_buf.at[0, pl.ds(mb * n_half, n_half)], h_buf.at[mb], gain_f)

    @pl.when(last)
    def _():
        for mb in range(2):
            part = pl.ds(mb * n_half, n_half)
            norm_into(n_buf.at[0, part], x_out.at[mb, body_rows], gain_h)
            e_on(mb).wait_recv()
            shape = (n_half, e_buf.shape[1])
            shifted = lax.broadcasted_iota(jnp.int32, shape, 1) == lax.broadcasted_iota(jnp.int32, shape, 0) + 1
            hot = jnp.where(shifted, 1.0, 0.0).astype(jnp.bfloat16)
            for n in range(0, width, HALF):
                n_buf[1, part, pl.ds(n, HALF)] = dot(hot, e_buf[mb, :, pl.ds(n, HALF)]).astype(jnp.bfloat16)
            norm_into(n_buf.at[1, part], n_buf.at[1, part], gain_e)

        def proj(g, c2):
            wait_slot(2 * g)
            wait_slot(2 * g + 1)
            for n in range(0, CHUNK, HALF):
                y = dot(n_buf[0], wbuf[2 * g, :, pl.ds(n, HALF)]) + dot(n_buf[1], wbuf[2 * g + 1, :, pl.ds(n, HALF)])
                at = pl.ds(pl.multiple_of(g * CHUNK + n, HALF), HALF)
                for mb in range(2):
                    z_buf[mb, body_rows, at] = y[mb * n_half : (mb + 1) * n_half].astype(jnp.bfloat16)
            issue_post(12 + 2 * g)
            issue_post(13 + 2 * g)
            return c2

        lax.fori_loop(0, 2, proj, 0)
        for mb in range(2):
            norm_into(n_buf.at[0, pl.ds(mb * n_half, n_half)], z_buf.at[mb, body_rows], gain_m)

        def up(i, c2):
            wait_slot(4 + i)
            for n in range(0, CHUNK, HALF):
                y = dot(n_buf[0], wbuf[4 + i, :, pl.ds(n, HALF)])
                hid[:, pl.ds(pl.multiple_of(i * CHUNK + n, HALF), HALF)] = gelu(y)
            issue_post(16 + i)
            return c2

        lax.fori_loop(0, 8, up, 0)

        def down(g, c2):
            for k in range(4):
                wait_slot(4 * g + k)
            for n in range(0, CHUNK, HALF):
                y = None
                for k in range(4):
                    part = dot(hid[:, pl.ds(k * width, width)], wbuf[4 * g + k, :, pl.ds(n, HALF)])
                    y = part if y is None else y + part
                at = pl.ds(pl.multiple_of(g * CHUNK + n, HALF), HALF)
                for mb in range(2):
                    part = y[mb * n_half : (mb + 1) * n_half]
                    z_buf[mb, body_rows, at] = (z_buf[mb, body_rows, at].astype(jnp.float32) + part).astype(jnp.bfloat16)
            for k in range(4):
                issue_post(24 + 4 * g + k)
            z_to_one(g).start()
            z_to_two(g).start()
            return c2

        lax.fori_loop(0, 2, down, 0)

    top[...] = jnp.full(top.shape, NEG, jnp.float32)
    total[...] = jnp.zeros(total.shape, jnp.float32)
    pick[...] = jnp.zeros(pick.shape, jnp.float32)
    lane = lax.broadcasted_iota(jnp.int32, (n_rows, LANES), 1)

    def head(which):
        def step(q, c2):
            slot = lax.rem(q, N_SLOTS)
            wait_slot(slot)
            col = head_col(q)
            low = col * CHUNK
            first = head_start(col)
            for n in range(0, CHUNK, HALF):
                y = dot(n_buf[which], wbuf[slot, :, pl.ds(n, HALF)])
                skip = low - (first + n)
                rel = tgt[which] - (first + n)
                rel = jnp.where(rel >= skip, rel, -1)
                old = top[which]
                picked = pick[which]
                parts = []
                for c in range(0, HALF, LANES):
                    part = jnp.where(lane >= skip - c, y[:, c : c + LANES], NEG)
                    picked = picked + jnp.where(lane == rel - c, part, 0.0)
                    parts.append(part)
                new = functools.reduce(jnp.maximum, parts, old)
                acc = total[which] * jnp.exp(old - new)
                for part in parts:
                    acc = acc + jnp.exp(part - new)
                top[which] = new
                total[which] = acc
                pick[which] = picked
            issue_post(q + N_SLOTS)
            return c2

        return step

    lax.fori_loop(0, n_main, head(0), 0)

    @pl.when(role < last_role)
    def _():
        for g in range(2):
            z_to_one(g).wait_recv()

            @pl.when(role == 1)
            def _():
                z_relay(g).start()

    for mb in range(2):
        norm_into(n_buf.at[1, pl.ds(mb * n_half, n_half)], z_buf.at[mb, body_rows], gain_f)
    lax.fori_loop(q_mtp, q_end, head(1), 0)

    for which in range(2):
        m = top[which]
        row_m = jnp.max(m, axis=1, keepdims=True)
        row_s = jnp.sum(total[which] * jnp.exp(m - row_m), axis=1, keepdims=True)
        row_p = jnp.sum(pick[which], axis=1, keepdims=True)
        packed = jnp.where(lane == 0, row_m, jnp.where(lane == 1, row_s, jnp.where(lane == 2, row_p, 0.0)))
        stat[me, which] = packed.T[:8]

    def stats_to(o):
        peer = lax.rem(me + o, n_dev)
        return remote(stat.at[me], stat.at[me], ss_sem.at[o], sr_sem.at[o], peer // n_roles, lax.rem(peer, n_roles))

    def stats_from(o):
        source = lax.rem(me + n_dev - o, n_dev)
        return remote(stat.at[me], stat.at[source], ss_sem.at[o], sr_sem.at[o], dp, role)

    for o in range(1, n_dev):
        stats_to(o).start()

    @pl.when(role == 0)
    def _():
        for mb in range(2):
            exchange(mb).wait_send()

    for mb in range(2):
        for g in range(2):

            @pl.when(role < last_role)
            def _():
                hand_on(mb, g).wait_send()

            @pl.when(last)
            def _():
                h_to_one(mb, g).wait_send()
                h_to_two(mb, g).wait_send()

            @pl.when(role == 1)
            def _():
                h_relay(mb, g).wait_send()

    for g in range(2):

        @pl.when(last)
        def _():
            z_to_one(g).wait_send()
            z_to_two(g).wait_send()

        @pl.when(role == 1)
        def _():
            z_relay(g).wait_send()

    for o in range(1, n_dev):
        stats_from(o).wait_recv()
    for o in range(1, n_dev):
        stats_to(o).wait_send()

    def nll(data, which):
        s = [stat[data * n_roles + r, which] for r in range(n_roles)]
        m = functools.reduce(jnp.maximum, [v[0:1] for v in s])
        t = sum(v[1:2] * jnp.exp(v[0:1] - m) for v in s)
        return m + jnp.log(t) - sum(v[2:3] for v in s)

    n_all = n_data * n_rows
    loss = jnp.zeros((1, 1), jnp.float32)
    for data in range(n_data):
        loss = loss + jnp.sum(nll(data, 0), axis=1, keepdims=True) + MTP_WEIGHT * jnp.sum(nll(data, 1), axis=1, keepdims=True)
    out[0:1] = nll(dp, 0)
    out[1:2] = nll(dp, 1)
    out[2:3] = jnp.broadcast_to(loss / n_all, (1, n_rows))
    out[3:8] = jnp.zeros((5, n_rows), jnp.float32)


def run_mega(rows, tgt, gains, weights):
    n_ext, width = rows.shape[1], rows.shape[2]
    n_rows = tgt.shape[1]
    n_half = n_rows // 2
    ffn = weights[0].shape[3]
    bf16, f32 = jnp.bfloat16, jnp.float32
    vmem = pl.BlockSpec(memory_space=pltpu.VMEM)
    anywhere = pl.BlockSpec(memory_space=pl.ANY)
    dma = pltpu.SemaphoreType.DMA
    return pl.pallas_call(
        mega_kernel,
        in_specs=[anywhere, vmem, vmem, vmem, vmem, vmem] + [anywhere] * 6,
        out_specs=vmem,
        out_shape=jax.ShapeDtypeStruct((8, n_rows), f32),
        scratch_shapes=[
            pltpu.VMEM((N_SLOTS, width, CHUNK), bf16),
            pltpu.VMEM((2, n_ext, width), bf16),
            pltpu.VMEM((n_rows, ffn), bf16),
            pltpu.VMEM((2, n_ext, width), bf16),
            pltpu.VMEM((2, n_half, width), bf16),
            pltpu.VMEM((2, n_ext, width), bf16),
            pltpu.VMEM((2, n_rows, width), bf16),
            pltpu.VMEM((2, n_rows, LANES), f32),
            pltpu.VMEM((2, n_rows, LANES), f32),
            pltpu.VMEM((2, n_rows, LANES), f32),
            pltpu.VMEM((8, 2, 8, n_rows), f32),
            dma((N_SLOTS,)),
            dma((2,)), dma((4,)), dma((4,)), dma((2,)), dma((2,)), dma((2,)), dma((2,)),
            dma((4,)), dma((4,)), dma((4,)), dma((4,)),
            dma((2,)), dma((2,)), dma((2,)), dma((2,)),
            dma((8,)), dma((8,)),
        ],
        compiler_params=pltpu.CompilerParams(collective_id=0, has_side_effects=True, vmem_limit_bytes=67043328),
        name="mega",
    )(rows, tgt, *gains, *weights)


def solution(mesh):
    n_data = mesh.shape['dp']
    swap = [(i, (i + 1) % n_data) for i in range(n_data)]

    def body(tok_ids, emb_s, w_one, w_two, gain_f, gain_h, gain_e, gain_m, w_proj, u_one, u_two, w_out):
        role = lax.axis_index('pp')
        dp = lax.axis_index('dp')
        n_micro, batch_dev, seq_plus = tok_ids.shape
        seq_len = seq_plus - 2
        n_seq = n_micro * batch_dev
        table = emb_s[0]
        shard_rows = table.shape[0]
        seqs = tok_ids.reshape(n_seq, seq_plus)
        ids_mine = seqs[:, : seq_len + 1]
        ids_other = lax.ppermute(ids_mine, 'dp', swap)
        ids = jnp.concatenate([ids_mine, ids_other]) - dp * shard_rows
        owned = (ids >= 0) & (ids < shard_rows)
        rows = gather_rows(role, jnp.clip(ids, 0, shard_rows - 1), owned, table)
        targets = jnp.stack([seqs[:, 1 : seq_len + 1].reshape(-1), seqs[:, 2:].reshape(-1)])
        tgt = jnp.broadcast_to(targets[:, :, None], targets.shape + (LANES,))
        gains = [gain_f, gain_h, gain_e, gain_m]
        out = run_mega(rows, tgt, gains, [w_one, w_two, w_proj, u_one, u_two, w_out])
        main_nll = out[0].reshape(n_micro, batch_dev, seq_len)
        mtp_nll = out[1].reshape(n_micro, batch_dev, seq_len)
        return out[2, 0], main_nll, mtp_nll

    replicated = P()
    in_specs = (P(None, 'dp', None), P('pp', 'dp', None), P('pp'), P('pp'), replicated, replicated, replicated, replicated, replicated, replicated, replicated, replicated)
    out_specs = (replicated, P(None, 'dp', None), P(None, 'dp', None))
    return jax.shard_map(body, mesh=mesh, in_specs=in_specs, out_specs=out_specs, check_vma=False)
```

```python
import functools

import jax
import jax.numpy as jnp
from jax import lax
from jax.experimental import pallas as pl
from jax.experimental.pallas import tpu as pltpu
from jax.sharding import PartitionSpec as P

NORM_EPS = 1e-6
MTP_WEIGHT = 0.3
LANES = 128
NEG = -3.0e38
CHUNK = 1024
HALF = 512
N_SLOTS = 12
MESH = pl.DeviceIdType.MESH
GROUP = 8
MAIN_SHARE = 32
MTP_SHARE = 24


def gather_kernel(n_ids, flag_ref, grp_ref, count_ref, sel_ref, table_ref, out_ref, buf, rows, sems, out_sems):
    n_batches = buf.shape[0]

    def start(batch):
        def one(j, carry):
            grp = grp_ref[batch * n_ids + j]

            @pl.when(grp >= 0)
            def _():
                first = pl.multiple_of(grp * GROUP, GROUP)
                pltpu.make_async_copy(
                    table_ref.at[pl.ds(first, GROUP), :], buf.at[batch, j], sems.at[batch]
                ).start()

            return carry

        lax.fori_loop(0, n_ids, one, 0, unroll=43)

    def wait(batch):
        def one(j, carry):
            pltpu.make_async_copy(buf.at[batch, 0], buf.at[batch, 0], sems.at[batch]).wait()
            return carry

        lax.fori_loop(0, count_ref[batch], one, 0)

    @pl.when(flag_ref[0] == 0)
    def _():
        for batch in range(n_batches):
            def clear(j, carry):
                buf[batch, j] = jnp.zeros(buf.shape[2:], buf.dtype)
                return carry

            lax.fori_loop(0, n_ids, clear, 0, unroll=3)
            start(batch)
        col = lax.broadcasted_iota(jnp.int32, (out_ref.shape[1], n_ids * GROUP), 1)
        for batch in range(n_batches):
            wait(batch)
            hot = jnp.where(col == sel_ref[batch], 1.0, 0.0).astype(jnp.bfloat16)
            src = buf[batch].reshape(n_ids * GROUP, -1)
            rows[batch] = jnp.dot(hot, src, preferred_element_type=jnp.float32).astype(jnp.bfloat16)
            pltpu.make_async_copy(rows.at[batch], out_ref.at[batch], out_sems.at[batch]).start()
        for batch in range(n_batches):
            pltpu.make_async_copy(rows.at[batch], out_ref.at[batch], out_sems.at[batch]).wait()


def gather_rows(flag, local, owned, table):
    n_batches, n_ids = local.shape
    n_out = pl.cdiv(n_ids, GROUP) * GROUP
    width = table.shape[1]
    grp = local // GROUP
    sub = local - grp * GROUP
    grp = jnp.where(owned, grp, -1)
    sel = jnp.where(owned, jnp.arange(n_ids, dtype=jnp.int32) * GROUP + sub, -1)
    sel = jnp.pad(sel, ((0, 0), (0, n_out - n_ids)), constant_values=-1)
    return pl.pallas_call(
        functools.partial(gather_kernel, n_ids),
        grid_spec=pltpu.PrefetchScalarGridSpec(
            num_scalar_prefetch=3,
            grid=(),
            in_specs=[pl.BlockSpec(memory_space=pltpu.VMEM), pl.BlockSpec(memory_space=pl.ANY)],
            out_specs=pl.BlockSpec(memory_space=pltpu.HBM),
            scratch_shapes=[
                pltpu.VMEM((n_batches, n_ids, GROUP, width), table.dtype),
                pltpu.VMEM((n_batches, n_out, width), table.dtype),
                pltpu.SemaphoreType.DMA((n_batches,)),
                pltpu.SemaphoreType.DMA((n_batches,)),
            ],
        ),
        out_shape=jax.ShapeDtypeStruct((n_batches, n_out, width), table.dtype),
        compiler_params=pltpu.CompilerParams(vmem_limit_bytes=66_000_000),
        cost_estimate=pl.CostEstimate(
            flops=2 * n_batches * n_out * n_ids * GROUP * width * 8, bytes_accessed=n_batches * n_ids * GROUP * width * 2, transcendentals=0
        ),
        name="gather_rows",
    )(flag.reshape(1), grp.reshape(-1), jnp.sum(owned, axis=1, dtype=jnp.int32), sel[..., None], table)


def scaled_rows(rows, gain):
    x_f = rows.astype(jnp.float32)
    y = x_f * lax.rsqrt(jnp.mean(x_f * x_f, axis=-1, keepdims=True) + NORM_EPS)
    if gain is not None:
        y = y * gain
    return y.astype(jnp.bfloat16)


def norm_into(dst, src, gain_ref=None):
    gain = None if gain_ref is None else gain_ref[...].astype(jnp.float32).reshape(1, -1)
    for r in range(0, src.shape[0], 16):
        dst[pl.ds(r, 16), :] = scaled_rows(src[pl.ds(r, 16), :], gain)


def gelu(y):
    inner = y * (0.7978845608028654 + (0.7978845608028654 * 0.044715) * (y * y))
    return (y * (0.5 + 0.5 * jnp.tanh(inner))).astype(jnp.bfloat16)


def dot(a, b):
    return jnp.dot(a, b, preferred_element_type=jnp.float32)


def mega_kernel(
    rows, tgt, gain_f, gain_h, gain_e, gain_m, w_one, w_two, w_proj, u_one, u_two, w_out,
    out, wbuf, x_in, hid, x_out, h_buf, n_buf, top, total, pick, stat,
    wsem, loc_sem, xs_sem, xr_sem, ex_s, ex_r, es_sem, er_sem, hs_sem, hs2_sem, hr_sem, rl_sem, zs_sem, zs2_sem, zr_sem, zl_sem, zx_s, zx_r, hx_s, hx_r, el_sem, ss_sem, sr_sem,
):
    role = lax.axis_index('pp')
    dp = lax.axis_index('dp')
    n_roles, n_data = 4, 2
    n_dev = n_roles * n_data
    me = dp * n_roles + role
    n_vocab = w_out.shape[1]
    width = x_in.shape[2]
    n_half = n_buf.shape[1] // 2
    n_rows = n_buf.shape[1]
    n_cols = pl.cdiv(n_vocab, CHUNK)
    xn = n_buf.at[0, pl.ds(0, n_half)]
    body_rows = pl.ds(0, n_half)
    z_buf = x_in
    last_role = n_roles - 1
    last = role == last_role
    is_mtp = role >= n_roles - 2
    own = jnp.maximum(role - (n_roles - 2), 0)
    mate = jnp.where(role == last_role, last_role - 1, last_role)
    large = (n_cols * MAIN_SHARE) // 100
    small = (n_cols - 2 * large + 1) // 2
    main_at = jnp.where(is_mtp, 2 * large + own * small, role * large)
    n_main = jnp.where(is_mtp, jnp.where(last, n_cols - 2 * large - small, small), large)
    few = (n_cols * MTP_SHARE) // 100
    more = (n_cols - 2 * few + 1) // 2
    mtp_at = jnp.where(is_mtp, 2 * few + own * more, role * few)
    n_mtp = jnp.where(is_mtp, jnp.where(last, n_cols - 2 * few - more, more), few)
    q_main = jnp.where(is_mtp, 10, 0)
    q_mtp = q_main + n_main
    q_end = q_mtp + n_mtp

    def load(src, slot):
        pltpu.make_async_copy(src, wbuf.at[slot], wsem.at[slot]).start()

    def wait_slot(slot):
        pltpu.make_async_copy(w_proj.at[pl.ds(0, width), pl.ds(0, CHUNK)], wbuf.at[slot], wsem.at[slot]).wait()

    def cols(c):
        return pl.ds(pl.multiple_of(c * CHUNK, CHUNK), CHUNK)

    def rows_at(k):
        return pl.ds(pl.multiple_of(k * width, width), width)

    def up_chunk(c):
        return w_one.at[0, 0, :, cols(c)]

    def down_chunk(g, k):
        return w_two.at[0, 0, rows_at(k), cols(g)]

    def head_col(q):
        return jnp.where(q < q_mtp, main_at + q - q_main, mtp_at + q - q_mtp)

    def head_start(col):
        return pl.multiple_of(jnp.minimum(col * CHUNK, n_vocab - CHUNK), LANES)

    def issue_post(q):
        slot = lax.rem(q, N_SLOTS)

        @pl.when((q >= q_main) & (q < q_end))
        def _():
            load(w_out.at[:, pl.ds(head_start(head_col(q)), CHUNK)], slot)

        @pl.when(is_mtp & (q < 2))
        def _():
            load(w_proj.at[rows_at(q), cols(own)], slot)

        @pl.when(is_mtp & (q >= 2) & (q < 6))
        def _():
            load(u_one.at[:, cols(4 * own + q - 2)], slot)

        @pl.when(is_mtp & (q >= 6) & (q < 10))
        def _():
            load(u_two.at[rows_at(q - 6), cols(own)], slot)

    def remote(src, dst, send, recv, to_dp, to_pp):
        return pltpu.make_async_remote_copy(
            src_ref=src, dst_ref=dst, send_sem=send, recv_sem=recv, device_id=(to_dp, to_pp), device_id_type=MESH
        )

    for c in range(8):
        load(up_chunk(c), c // 2 if c % 2 == 0 else 8 + (c // 2))
    for c in range(4):
        load(down_chunk(c // 2, 2 * (c % 2)), 4 + c)

    barrier = pltpu.get_barrier_semaphore()
    for o in range(1, n_dev):
        peer = lax.rem(me + o, n_dev)
        pl.semaphore_signal(barrier, inc=1, device_id=(peer // n_roles, lax.rem(peer, n_roles)), device_id_type=MESH)
    pl.semaphore_wait(barrier, n_dev - 1)

    def exchange(mb):
        return remote(rows.at[2 + mb], x_in.at[mb], ex_s.at[mb], ex_r.at[mb], 1 - dp, 0)

    def local_rows(mb):
        return pltpu.make_async_copy(rows.at[mb], x_out.at[mb], loc_sem.at[mb])

    @pl.when(role == 0)
    def _():
        exchange(0).start()
        for mb in range(2):
            local_rows(mb).start()

    def piece(ref, mb, g):
        return ref.at[mb, body_rows, cols(g)]

    def hand_on(mb, g):
        i = 2 * mb + g
        return remote(piece(x_out, mb, g), piece(x_in, mb, g), xs_sem.at[i], xr_sem.at[i], dp, jnp.minimum(role + 1, last_role))

    def h_to_one(mb, g):
        i = 2 * mb + g
        return remote(piece(x_out, mb, g), piece(h_buf, mb, g), hs_sem.at[i], hr_sem.at[i], dp, 1)

    def h_to_two(mb, g):
        i = 2 * mb + g
        return remote(piece(x_out, mb, g), piece(h_buf, mb, g), hs2_sem.at[i], hr_sem.at[i], dp, 2)

    def h_relay(mb, g):
        i = 2 * mb + g
        return remote(piece(h_buf, mb, g), piece(h_buf, mb, g), rl_sem.at[i], hr_sem.at[i], dp, 0)

    def e_on(mb):
        return remote(x_in.at[mb], h_buf.at[mb], es_sem.at[mb], er_sem.at[mb], dp, last_role)

    def half_rows(mb):
        return pl.ds(mb * n_half, n_half)

    def en_relay(mb):
        part = n_buf.at[1, half_rows(mb)]
        return remote(part, part, el_sem.at[mb], er_sem.at[mb], dp, last_role - 1)

    @pl.when(last)
    def _():
        for mb in range(2):
            e_on(mb).wait_recv()
            shape = (n_half, h_buf.shape[1])
            shifted = lax.broadcasted_iota(jnp.int32, shape, 1) == lax.broadcasted_iota(jnp.int32, shape, 0) + 1
            hot = jnp.where(shifted, 1.0, 0.0).astype(jnp.bfloat16)
            for n in range(0, width, HALF):
                n_buf[1, half_rows(mb), pl.ds(n, HALF)] = dot(hot, h_buf[mb, :, pl.ds(n, HALF)]).astype(jnp.bfloat16)
            norm_into(n_buf.at[1, half_rows(mb)], n_buf.at[1, half_rows(mb)], gain_e)
            en_relay(mb).start()

    def stage_pass(mb, carry):
        @pl.when(role == 0)
        def _():
            local_rows(mb).wait()
            exchange(mb).wait_recv()

            @pl.when(mb == 0)
            def _():
                exchange(1).start()

            for r in range(0, x_in.shape[1], 8):
                at = pl.ds(r, 8)
                x_in[mb, at, :] = x_in[mb, at, :] + x_out[mb, at, :]

        @pl.when(role > 0)
        def _():
            for g in range(2):
                hand_on(mb, g).wait_recv()

        norm_into(xn, x_in.at[mb, body_rows])

        @pl.when(role == 0)
        def _():
            e_on(mb).start()

        def up(i, c2):
            @pl.when(mb == 0)
            def _():
                wait_slot(i)

            wait_slot(8 + i)
            for e, slot in ((0, i), (1, 8 + i)):
                for n in range(0, CHUNK, HALF):
                    y = dot(xn[...], wbuf[slot, :, pl.ds(n, HALF)])
                    at = pl.multiple_of((2 * i + e) * CHUNK + n, HALF)
                    hid[pl.ds(0, n_half), pl.ds(at, HALF)] = gelu(y)
            g2 = i // 2
            load(down_chunk(g2, 2 * lax.rem(i, 2) + 1), 8 + i)

            @pl.when(mb == 1)
            def _():
                issue_post(i)

            return c2

        lax.fori_loop(0, 4, up, 0)

        def down(g, c2):
            @pl.when(mb == 0)
            def _():
                wait_slot(4 + 2 * g)
                wait_slot(5 + 2 * g)

            wait_slot(8 + 2 * g)
            wait_slot(9 + 2 * g)
            slots = (4 + 2 * g, 8 + 2 * g, 5 + 2 * g, 9 + 2 * g)
            for n in range(0, CHUNK, HALF):
                y = None
                for k in range(4):
                    part = dot(hid[pl.ds(0, n_half), pl.ds(k * width, width)], wbuf[slots[k], :, pl.ds(n, HALF)])
                    y = part if y is None else y + part
                at = pl.ds(pl.multiple_of(g * CHUNK + n, HALF), HALF)
                x_out[mb, body_rows, at] = (x_in[mb, body_rows, at].astype(jnp.float32) + y).astype(jnp.bfloat16)

            @pl.when(mb == 0)
            def _():
                load(up_chunk(4 * g + 1), 8 + 2 * g)
                load(up_chunk(4 * g + 3), 9 + 2 * g)

            @pl.when(mb == 1)
            def _():
                issue_post(4 + 2 * g)
                issue_post(5 + 2 * g)
                issue_post(8 + 2 * g)
                issue_post(9 + 2 * g)

            @pl.when((role == 0) & (g == 1))
            def _():
                e_on(mb).wait_send()

            @pl.when(role < last_role)
            def _():
                hand_on(mb, g).start()

            @pl.when(last)
            def _():
                h_to_one(mb, g).start()
                h_to_two(mb, g).start()

            return c2

        lax.fori_loop(0, 2, down, 0)
        return carry

    lax.fori_loop(0, 2, stage_pass, 0)

    def z_half(g, n):
        return z_buf.at[:, body_rows, pl.ds(pl.multiple_of(g * CHUNK + n * HALF, HALF), HALF)]

    def z_to_one(g, n):
        return remote(z_half(g, n), z_half(g, n), zs_sem.at[n], zr_sem.at[2 * g + n], dp, 1)

    def z_to_peer(g, n):
        return remote(z_half(g, n), z_half(g, n), zs2_sem.at[n], zr_sem.at[2 * g + n], dp, mate)

    def z_relay(g, n):
        return remote(z_half(g, n), z_half(g, n), zl_sem.at[2 * g + n], zr_sem.at[2 * g + n], dp, 0)

    def zx(g):
        piece_g = z_buf.at[:, body_rows, cols(g)]
        return remote(piece_g, piece_g, zx_s.at[0], zx_r.at[0], dp, mate)

    def hx(g, i):
        piece_g = hid.at[:, cols(4 * g + i)]
        return remote(piece_g, piece_g, hx_s.at[i], hx_r.at[i], dp, mate)

    def norm_h(gain):
        for mb in range(2):

            @pl.when(last)
            def _():
                norm_into(n_buf.at[0, half_rows(mb)], x_out.at[mb, body_rows], gain)

            @pl.when(role < last_role)
            def _():
                norm_into(n_buf.at[0, half_rows(mb)], h_buf.at[mb, body_rows], gain)

    @pl.when(role < last_role)
    def _():
        for mb in range(2):
            for g in range(2):
                h_to_one(mb, g).wait_recv()

                @pl.when(role == 1)
                def _():
                    h_relay(mb, g).start()

    @pl.when(is_mtp)
    def _():
        for mb in range(2):

            @pl.when(role < last_role)
            def _():
                en_relay(mb).wait_recv()

            @pl.when(last)
            def _():
                en_relay(mb).wait_send()

        norm_h(gain_h)

        wait_slot(0)
        wait_slot(1)
        for n in range(0, CHUNK, HALF):
            y = dot(n_buf[0], wbuf[0, :, pl.ds(n, HALF)]) + dot(n_buf[1], wbuf[1, :, pl.ds(n, HALF)])
            at = pl.ds(pl.multiple_of(own * CHUNK + n, HALF), HALF)
            for mb in range(2):
                z_buf[mb, body_rows, at] = y[mb * n_half : (mb + 1) * n_half].astype(jnp.bfloat16)
        issue_post(12)
        issue_post(13)
        zx(own).start()
        zx(1 - own).wait_recv()
        for mb in range(2):
            norm_into(n_buf.at[0, half_rows(mb)], z_buf.at[mb, body_rows], gain_m)

        def up(i, c2):
            wait_slot(2 + i)
            for n in range(0, CHUNK, HALF):
                y = dot(n_buf[0], wbuf[2 + i, :, pl.ds(n, HALF)])
                hid[:, pl.ds(pl.multiple_of((4 * own + i) * CHUNK + n, HALF), HALF)] = gelu(y)
            issue_post(14 + i)
            hx(own, i).start()
            return c2

        lax.fori_loop(0, 4, up, 0)
        zx(own).wait_send()
        for i in range(4):
            hx(1 - own, i).wait_recv()
        for k in range(4):
            wait_slot(6 + k)
        for n in range(2):
            y = None
            for k in range(4):
                part = dot(hid[:, pl.ds(k * width, width)], wbuf[6 + k, :, pl.ds(n * HALF, HALF)])
                y = part if y is None else y + part
            at = pl.ds(pl.multiple_of(own * CHUNK + n * HALF, HALF), HALF)
            for mb in range(2):
                part = y[mb * n_half : (mb + 1) * n_half]
                z_buf[mb, body_rows, at] = (z_buf[mb, body_rows, at].astype(jnp.float32) + part).astype(jnp.bfloat16)
            z_to_one(own, n).start()
            z_to_peer(own, n).start()
        for k in range(4):
            issue_post(18 + k)

    norm_h(gain_f)

    top[...] = jnp.full(top.shape, NEG, jnp.float32)
    total[...] = jnp.zeros(total.shape, jnp.float32)
    pick[...] = jnp.zeros(pick.shape, jnp.float32)
    lane = lax.broadcasted_iota(jnp.int32, (n_rows, LANES), 1)

    def head(which):
        def step(q, c2):
            slot = lax.rem(q, N_SLOTS)
            wait_slot(slot)
            col = head_col(q)
            low = col * CHUNK
            first = head_start(col)
            for n in range(0, CHUNK, HALF):
                y = dot(n_buf[which], wbuf[slot, :, pl.ds(n, HALF)])
                skip = low - (first + n)
                rel = tgt[which] - (first + n)
                rel = jnp.where(rel >= skip, rel, -1)
                old = top[which]
                picked = pick[which]
                parts = []
                for c in range(0, HALF, LANES):
                    part = jnp.where(lane >= skip - c, y[:, c : c + LANES], NEG)
                    picked = picked + jnp.where(lane == rel - c, part, 0.0)
                    parts.append(part)
                new = functools.reduce(jnp.maximum, parts, old)
                acc = total[which] * jnp.exp(old - new)
                for part in parts:
                    acc = acc + jnp.exp(part - new)
                top[which] = new
                total[which] = acc
                pick[which] = picked
            issue_post(q + N_SLOTS)
            return c2

        return step

    lax.fori_loop(q_main, q_mtp, head(0), 0)

    @pl.when(is_mtp)
    def _():
        for n in range(2):
            z_to_peer(1 - own, n).wait_recv()

    @pl.when(role < n_roles - 2)
    def _():
        for n in range(2):
            for g in range(2):
                z_to_one(g, n).wait_recv()

                @pl.when(role == 1)
                def _():
                    z_relay(g, n).start()

    for mb in range(2):
        norm_into(n_buf.at[1, pl.ds(mb * n_half, n_half)], z_buf.at[mb, body_rows], gain_f)
    lax.fori_loop(q_mtp, q_end, head(1), 0)

    for which in range(2):
        m = top[which]
        row_m = jnp.max(m, axis=1, keepdims=True)
        row_s = jnp.sum(total[which] * jnp.exp(m - row_m), axis=1, keepdims=True)
        row_p = jnp.sum(pick[which], axis=1, keepdims=True)
        packed = jnp.where(lane == 0, row_m, jnp.where(lane == 1, row_s, jnp.where(lane == 2, row_p, 0.0)))
        stat[me, which] = packed.T[:8]

    def stats_to(o):
        peer = lax.rem(me + o, n_dev)
        return remote(stat.at[me], stat.at[me], ss_sem.at[o], sr_sem.at[o], peer // n_roles, lax.rem(peer, n_roles))

    def stats_from(o):
        source = lax.rem(me + n_dev - o, n_dev)
        return remote(stat.at[me], stat.at[source], ss_sem.at[o], sr_sem.at[o], dp, role)

    for o in range(1, n_dev):
        stats_to(o).start()

    @pl.when(role == 0)
    def _():
        for mb in range(2):
            exchange(mb).wait_send()

    for mb in range(2):
        for g in range(2):

            @pl.when(role < last_role)
            def _():
                hand_on(mb, g).wait_send()

            @pl.when(last)
            def _():
                h_to_one(mb, g).wait_send()
                h_to_two(mb, g).wait_send()

            @pl.when(role == 1)
            def _():
                h_relay(mb, g).wait_send()

    @pl.when(is_mtp)
    def _():
        for n in range(2):
            z_to_one(own, n).wait_send()
            z_to_peer(own, n).wait_send()
        for i in range(4):
            hx(own, i).wait_send()

    @pl.when(role == 1)
    def _():
        for g in range(2):
            for n in range(2):
                z_relay(g, n).wait_send()

    for o in range(1, n_dev):
        stats_from(o).wait_recv()
    for o in range(1, n_dev):
        stats_to(o).wait_send()

    def nll(data, which):
        s = [stat[data * n_roles + r, which] for r in range(n_roles)]
        m = functools.reduce(jnp.maximum, [v[0:1] for v in s])
        t = sum(v[1:2] * jnp.exp(v[0:1] - m) for v in s)
        return m + jnp.log(t) - sum(v[2:3] for v in s)

    n_all = n_data * n_rows
    loss = jnp.zeros((1, 1), jnp.float32)
    for data in range(n_data):
        loss = loss + jnp.sum(nll(data, 0), axis=1, keepdims=True) + MTP_WEIGHT * jnp.sum(nll(data, 1), axis=1, keepdims=True)
    out[0:1] = nll(dp, 0)
    out[1:2] = nll(dp, 1)
    out[2:3] = jnp.broadcast_to(loss / n_all, (1, n_rows))
    out[3:8] = jnp.zeros((5, n_rows), jnp.float32)


def run_mega(rows, tgt, gains, weights):
    n_ext, width = rows.shape[1], rows.shape[2]
    n_rows = tgt.shape[1]
    n_half = n_rows // 2
    ffn = weights[0].shape[3]
    bf16, f32 = jnp.bfloat16, jnp.float32
    vmem = pl.BlockSpec(memory_space=pltpu.VMEM)
    anywhere = pl.BlockSpec(memory_space=pl.ANY)
    dma = pltpu.SemaphoreType.DMA
    return pl.pallas_call(
        mega_kernel,
        in_specs=[anywhere, vmem, vmem, vmem, vmem, vmem] + [anywhere] * 6,
        out_specs=vmem,
        out_shape=jax.ShapeDtypeStruct((8, n_rows), f32),
        scratch_shapes=[
            pltpu.VMEM((N_SLOTS, width, CHUNK), bf16),
            pltpu.VMEM((2, n_ext, width), bf16),
            pltpu.VMEM((n_rows, ffn), bf16),
            pltpu.VMEM((2, n_ext, width), bf16),
            pltpu.VMEM((2, n_ext, width), bf16),
            pltpu.VMEM((2, n_rows, width), bf16),
            pltpu.VMEM((2, n_rows, LANES), f32),
            pltpu.VMEM((2, n_rows, LANES), f32),
            pltpu.VMEM((2, n_rows, LANES), f32),
            pltpu.VMEM((8, 2, 8, n_rows), f32),
            dma((N_SLOTS,)),
            dma((2,)), dma((4,)), dma((4,)), dma((2,)), dma((2,)), dma((2,)), dma((2,)),
            dma((4,)), dma((4,)), dma((4,)), dma((4,)),
            dma((2,)), dma((2,)), dma((4,)), dma((4,)),
            dma((1,)), dma((1,)), dma((4,)), dma((4,)), dma((2,)),
            dma((8,)), dma((8,)),
        ],
        compiler_params=pltpu.CompilerParams(collective_id=0, has_side_effects=True, vmem_limit_bytes=67043328),
        name="mega",
    )(rows, tgt, *gains, *weights)


def solution(mesh):
    n_data = mesh.shape['dp']
    swap = [(i, (i + 1) % n_data) for i in range(n_data)]

    def body(tok_ids, emb_s, w_one, w_two, gain_f, gain_h, gain_e, gain_m, w_proj, u_one, u_two, w_out):
        role = lax.axis_index('pp')
        dp = lax.axis_index('dp')
        n_micro, batch_dev, seq_plus = tok_ids.shape
        seq_len = seq_plus - 2
        n_seq = n_micro * batch_dev
        table = emb_s[0]
        shard_rows = table.shape[0]
        seqs = tok_ids.reshape(n_seq, seq_plus)
        ids_mine = seqs[:, : seq_len + 1]
        ids_other = lax.ppermute(ids_mine, 'dp', swap)

        local = jnp.concatenate([ids_mine, ids_other]) - dp * shard_rows
        rows = gather_rows(role, jnp.clip(local, 0, shard_rows - 1), (local >= 0) & (local < shard_rows), table)
        targets = jnp.stack([seqs[:, 1 : seq_len + 1].reshape(-1), seqs[:, 2:].reshape(-1)])
        tgt = jnp.broadcast_to(targets[:, :, None], targets.shape + (LANES,))
        gains = [gain_f, gain_h, gain_e, gain_m]
        out = run_mega(rows, tgt, gains, [w_one, w_two, w_proj, u_one, u_two, w_out])
        main_nll = out[0].reshape(n_micro, batch_dev, seq_len)
        mtp_nll = out[1].reshape(n_micro, batch_dev, seq_len)
        return out[2, 0], main_nll, mtp_nll

    replicated = P()
    in_specs = (P(None, 'dp', None), P('pp', 'dp', None), P('pp'), P('pp'), replicated, replicated, replicated, replicated, replicated, replicated, replicated, replicated)
    out_specs = (replicated, P(None, 'dp', None), P(None, 'dp', None))
    return jax.shard_map(body, mesh=mesh, in_specs=in_specs, out_specs=out_specs, check_vma=False)
```

```python
import functools

import jax
import jax.numpy as jnp
from jax import lax
from jax.experimental import pallas as pl
from jax.experimental.pallas import tpu as pltpu
from jax.sharding import PartitionSpec as P

NORM_EPS = 1e-6
MTP_WEIGHT = 0.3
LANES = 128
NEG = -3.0e38
CHUNK = 1024
HALF = 512
N_SLOTS = 12
MESH = pl.DeviceIdType.MESH
GROUP = 8
MAIN_SHARE = 32
MTP_SHARE = 24


def gather_kernel(n_ids, flag_ref, grp_ref, count_ref, sel_ref, table_ref, out_ref, buf, rows, sems, out_sems):
    n_batches = buf.shape[0]

    def start(batch):
        def one(j, carry):
            grp = grp_ref[batch * n_ids + j]

            @pl.when(grp >= 0)
            def _():
                first = pl.multiple_of(grp * GROUP, GROUP)
                pltpu.make_async_copy(
                    table_ref.at[pl.ds(first, GROUP), :], buf.at[batch, j], sems.at[batch]
                ).start()

            return carry

        lax.fori_loop(0, n_ids, one, 0, unroll=43)

    def wait(batch):
        def one(j, carry):
            pltpu.make_async_copy(buf.at[batch, 0], buf.at[batch, 0], sems.at[batch]).wait()
            return carry

        lax.fori_loop(0, count_ref[batch], one, 0)

    @pl.when(flag_ref[0] == 0)
    def _():
        for batch in range(n_batches):
            def clear(j, carry):
                buf[batch, j] = jnp.zeros(buf.shape[2:], buf.dtype)
                return carry

            lax.fori_loop(0, n_ids, clear, 0, unroll=3)
            start(batch)
        col = lax.broadcasted_iota(jnp.int32, (out_ref.shape[1], n_ids * GROUP), 1)
        for batch in range(n_batches):
            wait(batch)
            hot = jnp.where(col == sel_ref[batch], 1.0, 0.0).astype(jnp.bfloat16)
            src = buf[batch].reshape(n_ids * GROUP, -1)
            rows[batch] = jnp.dot(hot, src, preferred_element_type=jnp.float32).astype(jnp.bfloat16)
            pltpu.make_async_copy(rows.at[batch], out_ref.at[batch], out_sems.at[batch]).start()
        for batch in range(n_batches):
            pltpu.make_async_copy(rows.at[batch], out_ref.at[batch], out_sems.at[batch]).wait()


def gather_rows(flag, local, owned, table):
    n_batches, n_ids = local.shape
    n_out = pl.cdiv(n_ids, GROUP) * GROUP
    width = table.shape[1]
    grp = local // GROUP
    sub = local - grp * GROUP
    grp = jnp.where(owned, grp, -1)
    sel = jnp.where(owned, jnp.arange(n_ids, dtype=jnp.int32) * GROUP + sub, -1)
    sel = jnp.pad(sel, ((0, 0), (0, n_out - n_ids)), constant_values=-1)
    return pl.pallas_call(
        functools.partial(gather_kernel, n_ids),
        grid_spec=pltpu.PrefetchScalarGridSpec(
            num_scalar_prefetch=3,
            grid=(),
            in_specs=[pl.BlockSpec(memory_space=pltpu.VMEM), pl.BlockSpec(memory_space=pl.ANY)],
            out_specs=pl.BlockSpec(memory_space=pltpu.HBM),
            scratch_shapes=[
                pltpu.VMEM((n_batches, n_ids, GROUP, width), table.dtype),
                pltpu.VMEM((n_batches, n_out, width), table.dtype),
                pltpu.SemaphoreType.DMA((n_batches,)),
                pltpu.SemaphoreType.DMA((n_batches,)),
            ],
        ),
        out_shape=jax.ShapeDtypeStruct((n_batches, n_out, width), table.dtype),
        compiler_params=pltpu.CompilerParams(vmem_limit_bytes=66_000_000),
        cost_estimate=pl.CostEstimate(
            flops=2 * n_batches * n_out * n_ids * GROUP * width * 8, bytes_accessed=n_batches * n_ids * GROUP * width * 2, transcendentals=0
        ),
        name="gather_rows",
    )(flag.reshape(1), grp.reshape(-1), jnp.sum(owned, axis=1, dtype=jnp.int32), sel[..., None], table)


def scaled_rows(rows, gain):
    x_f = rows.astype(jnp.float32)
    y = x_f * lax.rsqrt(jnp.mean(x_f * x_f, axis=-1, keepdims=True) + NORM_EPS)
    if gain is not None:
        y = y * gain
    return y.astype(jnp.bfloat16)


def norm_into(dst, src, gain_ref=None):
    gain = None if gain_ref is None else gain_ref[...].astype(jnp.float32).reshape(1, -1)
    for r in range(0, src.shape[0], 16):
        dst[pl.ds(r, 16), :] = scaled_rows(src[pl.ds(r, 16), :], gain)


def gelu(y):
    inner = y * (0.7978845608028654 + (0.7978845608028654 * 0.044715) * (y * y))
    return (y * (0.5 + 0.5 * jnp.tanh(inner))).astype(jnp.bfloat16)


def dot(a, b):
    return jnp.dot(a, b, preferred_element_type=jnp.float32)


def mega_kernel(
    rows, tgt, gain_f, gain_h, gain_e, gain_m, w_one, w_two, w_proj, u_one, u_two, w_out,
    out, wbuf, x_in, hid, x_out, h_buf, n_buf, top, total, pick, stat,
    wsem, loc_sem, xs_sem, xr_sem, ex_s, ex_r, es_sem, er_sem, hs_sem, hs2_sem, hr_sem, rl_sem, zs_sem, zs2_sem, zr_sem, zl_sem, zx_s, zx_r, hx_s, hx_r, el_sem, ss_sem, sr_sem,
):
    role = lax.axis_index('pp')
    dp = lax.axis_index('dp')
    n_roles, n_data = 4, 2
    n_dev = n_roles * n_data
    me = dp * n_roles + role
    n_vocab = w_out.shape[1]
    width = x_in.shape[2]
    n_half = n_buf.shape[1] // 2
    n_rows = n_buf.shape[1]
    n_cols = pl.cdiv(n_vocab, CHUNK)
    xn = n_buf.at[0, pl.ds(0, n_half)]
    body_rows = pl.ds(0, n_half)
    z_buf = x_in
    last_role = n_roles - 1
    last = role == last_role
    is_mtp = role >= n_roles - 2
    own = jnp.maximum(role - (n_roles - 2), 0)
    mate = jnp.where(role == last_role, last_role - 1, last_role)
    large = (n_cols * MAIN_SHARE) // 100
    small = (n_cols - 2 * large + 1) // 2
    main_at = jnp.where(is_mtp, 2 * large + own * small, role * large)
    n_main = jnp.where(is_mtp, jnp.where(last, n_cols - 2 * large - small, small), large)
    few = (n_cols * MTP_SHARE) // 100
    more = (n_cols - 2 * few + 1) // 2
    mtp_at = jnp.where(is_mtp, 2 * few + own * more, role * few)
    n_mtp = jnp.where(is_mtp, jnp.where(last, n_cols - 2 * few - more, more), few)
    q_main = jnp.where(is_mtp, 10, 0)
    q_mtp = q_main + n_main
    q_end = q_mtp + n_mtp

    def load(src, slot):
        pltpu.make_async_copy(src, wbuf.at[slot], wsem.at[slot]).start()

    def wait_slot(slot):
        pltpu.make_async_copy(w_proj.at[pl.ds(0, width), pl.ds(0, CHUNK)], wbuf.at[slot], wsem.at[slot]).wait()

    def cols(c):
        return pl.ds(pl.multiple_of(c * CHUNK, CHUNK), CHUNK)

    def rows_at(k):
        return pl.ds(pl.multiple_of(k * width, width), width)

    def up_chunk(c):
        return w_one.at[0, 0, :, cols(c)]

    def down_chunk(g, k):
        return w_two.at[0, 0, rows_at(k), cols(g)]

    def head_col(q):
        return jnp.where(q < q_mtp, main_at + q - q_main, mtp_at + q - q_mtp)

    def head_start(col):
        return pl.multiple_of(jnp.minimum(col * CHUNK, n_vocab - CHUNK), LANES)

    def issue_post(q):
        slot = lax.rem(q, N_SLOTS)

        @pl.when((q >= q_main) & (q < q_end))
        def _():
            load(w_out.at[:, pl.ds(head_start(head_col(q)), CHUNK)], slot)

        @pl.when(is_mtp & (q < 2))
        def _():
            load(w_proj.at[rows_at(q), cols(own)], slot)

        @pl.when(is_mtp & (q >= 2) & (q < 6))
        def _():
            load(u_one.at[:, cols(4 * own + q - 2)], slot)

        @pl.when(is_mtp & (q >= 6) & (q < 10))
        def _():
            load(u_two.at[rows_at(q - 6), cols(own)], slot)

    def remote(src, dst, send, recv, to_dp, to_pp):
        return pltpu.make_async_remote_copy(
            src_ref=src, dst_ref=dst, send_sem=send, recv_sem=recv, device_id=(to_dp, to_pp), device_id_type=MESH
        )

    def first_loads(chunks):
        for c in chunks:
            load(up_chunk(c), c // 2 if c % 2 == 0 else 8 + (c // 2))

    first_loads(range(2))

    barrier = pltpu.get_barrier_semaphore()
    for o in range(1, n_dev):
        peer = lax.rem(me + o, n_dev)
        pl.semaphore_signal(barrier, inc=1, device_id=(peer // n_roles, lax.rem(peer, n_roles)), device_id_type=MESH)
    pl.semaphore_wait(barrier, n_dev - 1)

    def exchange(mb):
        return remote(rows.at[2 + mb], x_in.at[mb], ex_s.at[mb], ex_r.at[mb], 1 - dp, 0)

    def local_rows(mb):
        return pltpu.make_async_copy(rows.at[mb], x_out.at[mb], loc_sem.at[mb])

    @pl.when(role == 0)
    def _():
        for mb in range(2):
            exchange(mb).start()
        for mb in range(2):
            local_rows(mb).start()

    first_loads(range(2, 8))
    for c in range(4):
        load(down_chunk(c // 2, 2 * (c % 2)), 4 + c)

    def piece(ref, mb, g):
        return ref.at[mb, body_rows, cols(g)]

    def hand_on(mb, g):
        i = 2 * mb + g
        return remote(piece(x_out, mb, g), piece(x_in, mb, g), xs_sem.at[i], xr_sem.at[i], dp, jnp.minimum(role + 1, last_role))

    def h_to_one(mb, g):
        i = 2 * mb + g
        return remote(piece(x_out, mb, g), piece(h_buf, mb, g), hs_sem.at[i], hr_sem.at[i], dp, 1)

    def h_to_two(mb, g):
        i = 2 * mb + g
        return remote(piece(x_out, mb, g), piece(h_buf, mb, g), hs2_sem.at[i], hr_sem.at[i], dp, 2)

    def h_relay(mb, g):
        i = 2 * mb + g
        return remote(piece(h_buf, mb, g), piece(h_buf, mb, g), rl_sem.at[i], hr_sem.at[i], dp, 0)

    def e_on(mb):
        return remote(x_in.at[mb], h_buf.at[mb], es_sem.at[mb], er_sem.at[mb], dp, last_role)

    def half_rows(mb):
        return pl.ds(mb * n_half, n_half)

    def en_relay(mb):
        part = n_buf.at[1, half_rows(mb)]
        return remote(part, part, el_sem.at[mb], er_sem.at[mb], dp, last_role - 1)

    @pl.when(last)
    def _():
        for mb in range(2):
            e_on(mb).wait_recv()
            shape = (n_half, h_buf.shape[1])
            shifted = lax.broadcasted_iota(jnp.int32, shape, 1) == lax.broadcasted_iota(jnp.int32, shape, 0) + 1
            hot = jnp.where(shifted, 1.0, 0.0).astype(jnp.bfloat16)
            for n in range(0, width, HALF):
                n_buf[1, half_rows(mb), pl.ds(n, HALF)] = dot(hot, h_buf[mb, :, pl.ds(n, HALF)]).astype(jnp.bfloat16)
            norm_into(n_buf.at[1, half_rows(mb)], n_buf.at[1, half_rows(mb)], gain_e)
            en_relay(mb).start()

    def stage_pass(mb, carry):
        @pl.when(role == 0)
        def _():
            local_rows(mb).wait()
            exchange(mb).wait_recv()
            for r in range(0, x_in.shape[1], 8):
                at = pl.ds(r, 8)
                x_in[mb, at, :] = x_in[mb, at, :] + x_out[mb, at, :]

        @pl.when(role > 0)
        def _():
            for g in range(2):
                hand_on(mb, g).wait_recv()

        norm_into(xn, x_in.at[mb, body_rows])

        @pl.when(role == 0)
        def _():
            e_on(mb).start()

        def up(i, c2):
            @pl.when(mb == 0)
            def _():
                wait_slot(i)

            wait_slot(8 + i)
            for e, slot in ((0, i), (1, 8 + i)):
                for n in range(0, CHUNK, HALF):
                    y = dot(xn[...], wbuf[slot, :, pl.ds(n, HALF)])
                    at = pl.multiple_of((2 * i + e) * CHUNK + n, HALF)
                    hid[pl.ds(0, n_half), pl.ds(at, HALF)] = gelu(y)
            g2 = i // 2
            load(down_chunk(g2, 2 * lax.rem(i, 2) + 1), 8 + i)
            return c2

        lax.fori_loop(0, 4, up, 0)

        def down(g, c2):
            @pl.when(mb == 0)
            def _():
                wait_slot(4 + 2 * g)
                wait_slot(5 + 2 * g)

            wait_slot(8 + 2 * g)
            wait_slot(9 + 2 * g)
            slots = (4 + 2 * g, 8 + 2 * g, 5 + 2 * g, 9 + 2 * g)
            for n in range(0, CHUNK, HALF):
                y = None
                for k in range(4):
                    part = dot(hid[pl.ds(0, n_half), pl.ds(k * width, width)], wbuf[slots[k], :, pl.ds(n, HALF)])
                    y = part if y is None else y + part
                at = pl.ds(pl.multiple_of(g * CHUNK + n, HALF), HALF)
                x_out[mb, body_rows, at] = (x_in[mb, body_rows, at].astype(jnp.float32) + y).astype(jnp.bfloat16)

            @pl.when(mb == 0)
            def _():
                load(up_chunk(4 * g + 1), 8 + 2 * g)
                load(up_chunk(4 * g + 3), 9 + 2 * g)

            @pl.when(mb == 1)
            def _():
                issue_post(2 * g)
                issue_post(2 * g + 1)
                issue_post(4 + 2 * g)
                issue_post(5 + 2 * g)
                issue_post(8 + 2 * g)
                issue_post(9 + 2 * g)

            @pl.when((role == 0) & (g == 1))
            def _():
                e_on(mb).wait_send()

            @pl.when(role < last_role)
            def _():
                hand_on(mb, g).start()

            @pl.when(last)
            def _():
                h_to_one(mb, g).start()
                h_to_two(mb, g).start()

            return c2

        lax.fori_loop(0, 2, down, 0)
        return carry

    lax.fori_loop(0, 2, stage_pass, 0)

    def z_half(g, n):
        return z_buf.at[:, body_rows, pl.ds(pl.multiple_of(g * CHUNK + n * HALF, HALF), HALF)]

    def z_to_one(g, n):
        return remote(z_half(g, n), z_half(g, n), zs_sem.at[n], zr_sem.at[2 * g + n], dp, 1)

    def z_to_peer(g, n):
        return remote(z_half(g, n), z_half(g, n), zs2_sem.at[n], zr_sem.at[2 * g + n], dp, mate)

    def z_relay(g, n):
        return remote(z_half(g, n), z_half(g, n), zl_sem.at[2 * g + n], zr_sem.at[2 * g + n], dp, 0)

    def zx(g):
        piece_g = z_buf.at[:, body_rows, cols(g)]
        return remote(piece_g, piece_g, zx_s.at[0], zx_r.at[0], dp, mate)

    def hx(g, i):
        piece_g = hid.at[:, cols(4 * g + i)]
        return remote(piece_g, piece_g, hx_s.at[i], hx_r.at[i], dp, mate)

    def norm_h(gain):
        for mb in range(2):

            @pl.when(last)
            def _():
                norm_into(n_buf.at[0, half_rows(mb)], x_out.at[mb, body_rows], gain)

            @pl.when(role < last_role)
            def _():
                norm_into(n_buf.at[0, half_rows(mb)], h_buf.at[mb, body_rows], gain)

    @pl.when(role < last_role)
    def _():
        for mb in range(2):
            for g in range(2):
                h_to_one(mb, g).wait_recv()

                @pl.when(role == 1)
                def _():
                    h_relay(mb, g).start()

    @pl.when(is_mtp)
    def _():
        for mb in range(2):

            @pl.when(role < last_role)
            def _():
                en_relay(mb).wait_recv()

            @pl.when(last)
            def _():
                en_relay(mb).wait_send()

        norm_h(gain_h)

        wait_slot(0)
        wait_slot(1)
        for n in range(0, CHUNK, HALF):
            y = dot(n_buf[0], wbuf[0, :, pl.ds(n, HALF)]) + dot(n_buf[1], wbuf[1, :, pl.ds(n, HALF)])
            at = pl.ds(pl.multiple_of(own * CHUNK + n, HALF), HALF)
            for mb in range(2):
                z_buf[mb, body_rows, at] = y[mb * n_half : (mb + 1) * n_half].astype(jnp.bfloat16)
        issue_post(12)
        issue_post(13)
        zx(own).start()
        zx(1 - own).wait_recv()
        for mb in range(2):
            norm_into(n_buf.at[0, half_rows(mb)], z_buf.at[mb, body_rows], gain_m)

        def up(i, c2):
            wait_slot(2 + i)
            for n in range(0, CHUNK, HALF):
                y = dot(n_buf[0], wbuf[2 + i, :, pl.ds(n, HALF)])
                hid[:, pl.ds(pl.multiple_of((4 * own + i) * CHUNK + n, HALF), HALF)] = gelu(y)
            issue_post(14 + i)
            hx(own, i).start()
            return c2

        lax.fori_loop(0, 4, up, 0)
        zx(own).wait_send()
        for i in range(4):
            hx(1 - own, i).wait_recv()
        for k in range(4):
            wait_slot(6 + k)
        for n in range(2):
            y = None
            for k in range(4):
                part = dot(hid[:, pl.ds(k * width, width)], wbuf[6 + k, :, pl.ds(n * HALF, HALF)])
                y = part if y is None else y + part
            at = pl.ds(pl.multiple_of(own * CHUNK + n * HALF, HALF), HALF)
            for mb in range(2):
                part = y[mb * n_half : (mb + 1) * n_half]
                z_buf[mb, body_rows, at] = (z_buf[mb, body_rows, at].astype(jnp.float32) + part).astype(jnp.bfloat16)
            z_to_one(own, n).start()
            z_to_peer(own, n).start()
        for k in range(4):
            issue_post(18 + k)

    norm_h(gain_f)

    top[...] = jnp.full(top.shape, NEG, jnp.float32)
    total[...] = jnp.zeros(total.shape, jnp.float32)
    pick[...] = jnp.zeros(pick.shape, jnp.float32)
    lane = lax.broadcasted_iota(jnp.int32, (n_rows, LANES), 1)

    def head(which):
        def step(q, c2):
            slot = lax.rem(q, N_SLOTS)
            wait_slot(slot)
            col = head_col(q)
            low = col * CHUNK
            first = head_start(col)
            for n in range(0, CHUNK, HALF):
                y = dot(n_buf[which], wbuf[slot, :, pl.ds(n, HALF)])
                skip = low - (first + n)
                rel = tgt[which] - (first + n)
                rel = jnp.where(rel >= skip, rel, -1)
                old = top[which]
                picked = pick[which]
                parts = []
                for c in range(0, HALF, LANES):
                    part = jnp.where(lane >= skip - c, y[:, c : c + LANES], NEG)
                    picked = picked + jnp.where(lane == rel - c, part, 0.0)
                    parts.append(part)
                new = functools.reduce(jnp.maximum, parts, old)
                acc = total[which] * jnp.exp(old - new)
                for part in parts:
                    acc = acc + jnp.exp(part - new)
                top[which] = new
                total[which] = acc
                pick[which] = picked
            issue_post(q + N_SLOTS)
            return c2

        return step

    lax.fori_loop(q_main, q_mtp, head(0), 0)

    @pl.when(is_mtp)
    def _():
        for n in range(2):
            z_to_peer(1 - own, n).wait_recv()

    @pl.when(role < n_roles - 2)
    def _():
        for n in range(2):
            for g in range(2):
                z_to_one(g, n).wait_recv()

                @pl.when(role == 1)
                def _():
                    z_relay(g, n).start()

    for mb in range(2):
        norm_into(n_buf.at[1, pl.ds(mb * n_half, n_half)], z_buf.at[mb, body_rows], gain_f)
    lax.fori_loop(q_mtp, q_end, head(1), 0)

    for which in range(2):
        m = top[which]
        row_m = jnp.max(m, axis=1, keepdims=True)
        row_s = jnp.sum(total[which] * jnp.exp(m - row_m), axis=1, keepdims=True)
        row_p = jnp.sum(pick[which], axis=1, keepdims=True)
        packed = jnp.where(lane == 0, row_m, jnp.where(lane == 1, row_s, jnp.where(lane == 2, row_p, 0.0)))
        stat[me, which] = packed.T[:8]

    def stats_to(o):
        peer = lax.rem(me + o, n_dev)
        return remote(stat.at[me], stat.at[me], ss_sem.at[o], sr_sem.at[o], peer // n_roles, lax.rem(peer, n_roles))

    def stats_from(o):
        source = lax.rem(me + n_dev - o, n_dev)
        return remote(stat.at[me], stat.at[source], ss_sem.at[o], sr_sem.at[o], dp, role)

    for o in range(1, n_dev):
        stats_to(o).start()

    @pl.when(role == 0)
    def _():
        for mb in range(2):
            exchange(mb).wait_send()

    for mb in range(2):
        for g in range(2):

            @pl.when(role < last_role)
            def _():
                hand_on(mb, g).wait_send()

            @pl.when(last)
            def _():
                h_to_one(mb, g).wait_send()
                h_to_two(mb, g).wait_send()

            @pl.when(role == 1)
            def _():
                h_relay(mb, g).wait_send()

    @pl.when(is_mtp)
    def _():
        for n in range(2):
            z_to_one(own, n).wait_send()
            z_to_peer(own, n).wait_send()
        for i in range(4):
            hx(own, i).wait_send()

    @pl.when(role == 1)
    def _():
        for g in range(2):
            for n in range(2):
                z_relay(g, n).wait_send()

    for o in range(1, n_dev):
        stats_from(o).wait_recv()
    for o in range(1, n_dev):
        stats_to(o).wait_send()

    def nll(data, which):
        s = [stat[data * n_roles + r, which] for r in range(n_roles)]
        m = functools.reduce(jnp.maximum, [v[0:1] for v in s])
        t = sum(v[1:2] * jnp.exp(v[0:1] - m) for v in s)
        return m + jnp.log(t) - sum(v[2:3] for v in s)

    n_all = n_data * n_rows
    loss = jnp.zeros((1, 1), jnp.float32)
    for data in range(n_data):
        loss = loss + jnp.sum(nll(data, 0), axis=1, keepdims=True) + MTP_WEIGHT * jnp.sum(nll(data, 1), axis=1, keepdims=True)
    out[0:1] = nll(dp, 0)
    out[1:2] = nll(dp, 1)
    out[2:3] = jnp.broadcast_to(loss / n_all, (1, n_rows))
    out[3:8] = jnp.zeros((5, n_rows), jnp.float32)


def run_mega(rows, tgt, gains, weights):
    n_ext, width = rows.shape[1], rows.shape[2]
    n_rows = tgt.shape[1]
    n_half = n_rows // 2
    ffn = weights[0].shape[3]
    bf16, f32 = jnp.bfloat16, jnp.float32
    vmem = pl.BlockSpec(memory_space=pltpu.VMEM)
    anywhere = pl.BlockSpec(memory_space=pl.ANY)
    dma = pltpu.SemaphoreType.DMA
    return pl.pallas_call(
        mega_kernel,
        in_specs=[anywhere, vmem, vmem, vmem, vmem, vmem] + [anywhere] * 6,
        out_specs=vmem,
        out_shape=jax.ShapeDtypeStruct((8, n_rows), f32),
        scratch_shapes=[
            pltpu.VMEM((N_SLOTS, width, CHUNK), bf16),
            pltpu.VMEM((2, n_ext, width), bf16),
            pltpu.VMEM((n_rows, ffn), bf16),
            pltpu.VMEM((2, n_ext, width), bf16),
            pltpu.VMEM((2, n_ext, width), bf16),
            pltpu.VMEM((2, n_rows, width), bf16),
            pltpu.VMEM((2, n_rows, LANES), f32),
            pltpu.VMEM((2, n_rows, LANES), f32),
            pltpu.VMEM((2, n_rows, LANES), f32),
            pltpu.VMEM((8, 2, 8, n_rows), f32),
            dma((N_SLOTS,)),
            dma((2,)), dma((4,)), dma((4,)), dma((2,)), dma((2,)), dma((2,)), dma((2,)),
            dma((4,)), dma((4,)), dma((4,)), dma((4,)),
            dma((2,)), dma((2,)), dma((4,)), dma((4,)),
            dma((1,)), dma((1,)), dma((4,)), dma((4,)), dma((2,)),
            dma((8,)), dma((8,)),
        ],
        compiler_params=pltpu.CompilerParams(collective_id=0, has_side_effects=True, vmem_limit_bytes=67043328),
        name="mega",
    )(rows, tgt, *gains, *weights)


def solution(mesh):
    n_data = mesh.shape['dp']
    swap = [(i, (i + 1) % n_data) for i in range(n_data)]

    def body(tok_ids, emb_s, w_one, w_two, gain_f, gain_h, gain_e, gain_m, w_proj, u_one, u_two, w_out):
        role = lax.axis_index('pp')
        dp = lax.axis_index('dp')
        n_micro, batch_dev, seq_plus = tok_ids.shape
        seq_len = seq_plus - 2
        n_seq = n_micro * batch_dev
        table = emb_s[0]
        shard_rows = table.shape[0]
        seqs = tok_ids.reshape(n_seq, seq_plus)
        ids_mine = seqs[:, : seq_len + 1]
        ids_other = lax.ppermute(ids_mine, 'dp', swap)

        local = jnp.concatenate([ids_mine, ids_other]) - dp * shard_rows
        rows = gather_rows(role, jnp.clip(local, 0, shard_rows - 1), (local >= 0) & (local < shard_rows), table)
        targets = jnp.stack([seqs[:, 1 : seq_len + 1].reshape(-1), seqs[:, 2:].reshape(-1)])
        tgt = jnp.broadcast_to(targets[:, :, None], targets.shape + (LANES,))
        gains = [gain_f, gain_h, gain_e, gain_m]
        out = run_mega(rows, tgt, gains, [w_one, w_two, w_proj, u_one, u_two, w_out])
        main_nll = out[0].reshape(n_micro, batch_dev, seq_len)
        mtp_nll = out[1].reshape(n_micro, batch_dev, seq_len)
        return out[2, 0], main_nll, mtp_nll

    replicated = P()
    in_specs = (P(None, 'dp', None), P('pp', 'dp', None), P('pp'), P('pp'), replicated, replicated, replicated, replicated, replicated, replicated, replicated, replicated)
    out_specs = (replicated, P(None, 'dp', None), P(None, 'dp', None))
    return jax.shard_map(body, mesh=mesh, in_specs=in_specs, out_specs=out_specs, check_vma=False)
```
